32 devices in a mesh: lon: 16 (over z, x, core), lat: 2 (over y).
Axes of the slice: x: 2, y: 2, z: 4, core: 2. Of those that a mesh axis runs over, the one named last changes fastest.
Arguments:
- fields: float32 [128, 64, 4, 768], P('lat', 'lon'), may hold values from -24 to 24
- norm_gains: float32 [4, 768], replicated, may hold values from 0.25 to 1.75
- qkv_weight: bfloat16 [3, 768, 2304], replicated, may hold values from -0.21875 to 0.21875
- out_weight: bfloat16 [3, 768, 768], replicated, may hold values from -0.21875 to 0.21875
- longitude_bias: float32 [12, 64], replicated, may hold values from -3 to 380
- latitude_bias: float32 [12, 255], replicated, may hold values from -3 to 380
- level_bias: float32 [12, 7], replicated, may hold values from -3 to 380
- mlp_in: bfloat16 [768, 3072], replicated, may hold values from -0.21875 to 0.21875
- mlp_out: bfloat16 [3072, 768], replicated, may hold values from -0.109375 to 0.109375
Outputs:
- block_out: float32 [128, 64, 4, 768], P('lat', 'lon')
The draws below stay inside these ranges and needn't reach their ends.
All inputs are finite; a program needn't handle non-finite values.
Results may differ from the reference program's by a relative error of at most 0.013.
Values may be sent and summed in bfloat16 or wider, within the bound.
A program may use at most 192 MiB of HBM per device.

```python
import jax
import jax.numpy as jnp
from jax import lax

D = 768
HEADS = 12
FF = 3072
LEV = 4
NLAT = 128
NLON = 64


def draw_fields(key, part):
    full_shape = (NLAT, NLON, LEV, D)
    key_base, key_rows, key_channels = jax.random.split(key, 3)
    random_part = jax.random.normal(key_base, full_shape, jnp.float32)
    row_scale = jnp.exp(jax.random.uniform(key_rows, (NLAT, NLON, LEV, 1), jnp.float32, jnp.log(0.3), jnp.log(3.0)))
    channels = jnp.exp(jax.random.uniform(key_channels, (D,), jnp.float32, jnp.log(0.3), jnp.log(3.0)))
    values = random_part * row_scale * channels
    return jnp.clip(values, -24.0, 24.0)


def plant(key, length):
    key_base = jax.random.fold_in(key, 0)
    lookup = jax.random.uniform(key_base, (HEADS, length), jnp.float32, -3.0, 3.0)
    return lookup


def draw_longitude_bias(key, part):
    return plant(jax.random.fold_in(key, 11), NLON)


def draw_latitude_bias(key, part):
    return plant(jax.random.fold_in(key, 12), 2 * NLAT - 1)


def draw_level_bias(key, part):
    return plant(jax.random.fold_in(key, 13), 2 * LEV - 1)


def scatter_about(stream_key, dims, spread, limit, kind=jnp.bfloat16):
    result = jax.random.normal(stream_key, dims, jnp.float32) * spread
    return jnp.minimum(jnp.maximum(result, -limit), limit).astype(kind)


def setup_inputs(seed: int = 0) -> dict:
    splits = jax.random.split(jax.random.key(seed), 10)
    return {
        "fields": draw_fields(jax.random.fold_in(splits[9], 71), 0),
        "norm_gains": jnp.clip(1.0 + 0.15 * jax.random.normal(splits[1], (4, D), jnp.float32), 0.25, 1.75),
        "qkv_weight": scatter_about(splits[2], (3, D, 3 * D), D ** -0.5, 0.21875),
        "out_weight": scatter_about(splits[3], (3, D, D), D ** -0.5, 0.21875),
        "longitude_bias": draw_longitude_bias(jax.random.fold_in(splits[9], 71), 0),
        "latitude_bias": draw_latitude_bias(jax.random.fold_in(splits[9], 71), 0),
        "level_bias": draw_level_bias(jax.random.fold_in(splits[9], 71), 0),
        "mlp_in": scatter_about(splits[7], (D, FF), D ** -0.5, 0.21875),
        "mlp_out": scatter_about(splits[8], (FF, D), FF ** -0.5, 0.109375),
    }


epsilon = 1e-06
group_rows = 8

def normalize(fields, gain_row):
    square = lax.optimization_barrier(jnp.mean(fields * fields, axis=-1, keepdims=True))
    return (fields * lax.rsqrt(square + epsilon) * gain_row).astype(jnp.bfloat16)

def project(fields, gain_row, weight):
    features = fields.shape[-1]
    normed = normalize(fields, gain_row).reshape(-1, features)
    projected = jnp.dot(normed, weight, preferred_element_type=jnp.float32).astype(jnp.bfloat16)
    head_shape = fields.shape[:-1] + (HEADS, features // HEADS)
    return tuple((projected[:, member * features:(member + 1) * features].reshape(head_shape) for member in range(3)))

def attend(queries, key_rows, values, position_bias, position):
    letters = ['a', 'b', 'c']
    query_form = ''.join(('i' if member == position else letters[member] for member in range(3)))
    key_form = ''.join(('j' if member == position else letters[member] for member in range(3)))
    batch_form = ''.join((letters[member] for member in range(3) if member != position))
    inverse_root = queries.shape[-1] ** (-0.5)
    scores = jnp.einsum(query_form + 'he,' + key_form + 'he->' + batch_form + 'hij', queries.astype(jnp.float32), key_rows.astype(jnp.float32))
    weights = jax.nn.softmax(scores * inverse_root + position_bias, axis=-1).astype(jnp.bfloat16)
    attended = jnp.einsum(batch_form + 'hij,' + key_form + 'he->' + query_form + 'he', weights.astype(jnp.float32), values.astype(jnp.float32))
    return attended.astype(jnp.bfloat16)

def finish(fields, attended, out_rows):
    features = fields.shape[-1]
    update = jnp.dot(attended.reshape(-1, features), out_rows, preferred_element_type=jnp.float32)
    return fields + update.reshape(fields.shape)

def sweep(fields, position, gain_row, qkv_rows, out_rows, position_bias):
    queries, key_rows, values = project(fields, gain_row, qkv_rows)
    return finish(fields, attend(queries, key_rows, values, position_bias, position), out_rows)

def feed_forward(fields, gain_row, weight_in, weight_out):
    features = fields.shape[-1]
    normed = normalize(fields, gain_row).reshape(-1, features)
    hidden = jax.nn.gelu(jnp.dot(normed, weight_in, preferred_element_type=jnp.float32), approximate=True).astype(jnp.bfloat16)
    return fields + jnp.dot(hidden, weight_out, preferred_element_type=jnp.float32).reshape(fields.shape)

def toeplitz(window, row_count, col_count):
    heads = window.shape[0]
    width = row_count + col_count - 1
    padded = jnp.concatenate([window, jnp.zeros((heads, 1), window.dtype)], axis=1)
    flat = jnp.tile(padded, (1, row_count))[:, :row_count * width]
    return flat.reshape(heads, row_count, width)[:, :, row_count - 1:]

def periodic_bias(lookup):
    length = lookup.shape[1]
    window = jnp.concatenate([lookup[:, 1:], lookup], axis=1)
    return toeplitz(window, length, length)

def open_bias(lookup, first_row, query_count):
    length = (lookup.shape[1] + 1) // 2
    start = length - query_count - first_row
    window = lax.dynamic_slice_in_dim(lookup, start, query_count + length - 1, 1)
    return toeplitz(window, query_count, length)

def in_groups(function, fields, mapped_axis):
    leading = jnp.moveaxis(fields, mapped_axis, 0)
    groups = leading.reshape((leading.shape[0] // group_rows, group_rows) + leading.shape[1:])
    outputs = lax.map(lambda pencils: jnp.moveaxis(function(jnp.moveaxis(pencils, 0, mapped_axis)), mapped_axis, 0), groups)
    return jnp.moveaxis(outputs.reshape(leading.shape), 0, mapped_axis)

def reference(fields, norm_gains, qkv_weight, out_weight, longitude_bias, latitude_bias, level_bias, mlp_in, mlp_out):
    beside_all = periodic_bias(longitude_bias)
    meridian = open_bias(latitude_bias, 0, NLAT)
    column = open_bias(level_bias, 0, LEV)
    state = in_groups(lambda pencils: sweep(pencils, 1, norm_gains[0], qkv_weight[0], out_weight[0], beside_all), fields, 0)
    state = in_groups(lambda pencils: sweep(pencils, 0, norm_gains[1], qkv_weight[1], out_weight[1], meridian), state, 1)

    def column_steps(pencils):
        pencils = sweep(pencils, 2, norm_gains[2], qkv_weight[2], out_weight[2], column)
        return feed_forward(pencils, norm_gains[3], mlp_in, mlp_out)
    return in_groups(column_steps, state, 0)
```

```python
import functools

import jax
import jax.numpy as jnp
from jax import lax
from jax.experimental import pallas as pl
from jax.experimental.pallas import tpu as pltpu
from jax.sharding import PartitionSpec as P

HEAD = 64
EPSILON = 1e-06
LANES = 128
BLOCK = 256
NEGATIVE = -1e30
BF16 = jnp.bfloat16
F32 = jnp.float32


def normalize(fields, gain_row):
    square = jnp.mean(fields * fields, axis=-1, keepdims=True)
    return (fields * lax.rsqrt(square + EPSILON) * gain_row).astype(BF16)


def gelu(u):
    inner = u * (0.7978845608028654 + (0.7978845608028654 * 0.044715) * (u * u))
    half = 0.5 * u
    return half + half * jnp.tanh(inner)


def sweep_block(state, gain_row, qkv_ref, out_ref, bias_ref, index, group):
    tokens, features = state.shape
    normed = normalize(state, gain_row)
    qkv = jnp.dot(normed, qkv_ref[index], preferred_element_type=F32).astype(BF16)
    low = lax.broadcasted_iota(jnp.int32, (group, LANES), 1) < HEAD
    zero = jnp.zeros((group, LANES), BF16)
    one = jnp.ones((group, LANES), BF16)
    sums = (jnp.where(low, one, zero), jnp.where(low, zero, one))
    scale = jnp.asarray(HEAD**-0.5, BF16)
    columns = []
    for pair in range(features // LANES):
        rows = []
        for start in range(0, tokens, group):
            here = slice(start, start + group)
            q = qkv[here, pair * LANES : (pair + 1) * LANES] * scale
            k = qkv[here, features + pair * LANES : features + (pair + 1) * LANES]
            v = qkv[here, 2 * features + pair * LANES : 2 * features + (pair + 1) * LANES]
            keys = jnp.concatenate([jnp.where(low, k, zero), jnp.where(low, zero, k)], axis=0)
            scores = lax.dot_general(
                q, keys, (((1,), (1,)), ((), ())), preferred_element_type=F32
            )
            scores = scores + bias_ref[pair]
            halves = []
            for head in range(2):
                part = scores[:, head * group : (head + 1) * group]
                peak = jnp.max(part, axis=-1, keepdims=True)
                halves.append(jnp.exp(part - peak).astype(BF16))
            values = jnp.concatenate(
                [
                    jnp.concatenate([jnp.where(low, v, zero), sums[0]], axis=1),
                    jnp.concatenate([jnp.where(low, zero, v), sums[1]], axis=1),
                ],
                axis=0,
            )
            summed = jnp.dot(
                jnp.concatenate(halves, axis=1), values, preferred_element_type=F32
            )
            rows.append((summed[:, :LANES] / summed[:, LANES:]).astype(BF16))
        columns.append(jnp.concatenate(rows, axis=0))
    attended = jnp.concatenate(columns, axis=1)
    return state + jnp.dot(attended, out_ref[index], preferred_element_type=F32)


def feed_forward(state, gain_row, in_ref, out_ref):
    features = state.shape[1]
    hidden_count = in_ref.shape[1]
    normed = normalize(state, gain_row)
    result = state
    for start in range(0, hidden_count, features):
        u = jnp.dot(normed, in_ref[:, start : start + features], preferred_element_type=F32)
        hidden = gelu(u).astype(BF16)
        result = result + jnp.dot(
            hidden, out_ref[start : start + features, :], preferred_element_type=F32
        )
    return result


def strided_rows(ref, start, count, stride):
    return jnp.concatenate(
        [ref[c, pl.ds(start, count, stride=stride), :] for c in range(ref.shape[0])], axis=1
    )


def folded_rows(ref, row, lev, count):
    return jnp.concatenate(
        [
            ref[c, pl.ds(row + half * lev, count, stride=2 * lev), :]
            for half in range(2)
            for c in range(ref.shape[0])
        ],
        axis=1,
    )


def store_strided(ref, start, count, stride, value):
    for c in range(ref.shape[0]):
        ref[c, pl.ds(start, count, stride=stride), :] = value[:, c * LANES : (c + 1) * LANES]


def fill_bias(table_ref, sweep, shift, bias_ref, length, group):
    heads = 2 * bias_ref.shape[0]
    width = table_ref.shape[2]
    rows = lax.broadcasted_iota(jnp.int32, (group, group), 0) // length
    cols = lax.broadcasted_iota(jnp.int32, (group, group), 1) // length
    for head in range(heads):
        line = jnp.broadcast_to(table_ref[sweep, head : head + 1, :], (group, width))
        line = pltpu.roll(line, shift % width, 1)
        rolled = pltpu.roll(line, 0, 1, stride=1, stride_axis=0)[:, :group]
        if length < group:
            rolled = jnp.where(rows == cols, rolled, NEGATIVE)
        bias_ref[head // 2, :, head % 2 * group : (head % 2 + 1) * group] = rolled


def kernel(
    sizes,
    x_ref, gains_ref, lon_ref, lat_ref, lev_ref, qkv_hbm, out_hbm, in_hbm, mlp_hbm,
    o_ref,
    qkv_ref, out_ref, in_ref, mlp_ref,
    table_ref, bias_lon, bias_lat, bias_lev,
    circ, outbox, mer, lane_row, lane_mer, lane_lev, last,
    weight_sem, send_a, recv_a, send_b, recv_b, send_c, recv_c,
):
    nlon, nlat, lev, lons, lats, rows, heads = sizes
    devices = lons * lats
    me_lon, me_lat = lax.axis_index("lon"), lax.axis_index("lat")
    me = me_lon * lats + me_lat
    local_lat = nlat // lats
    per_dest = nlon // devices
    own = local_lat * lev
    group_lon, group_lat = max(LANES, nlon), max(LANES, nlat)

    loads = []
    for s in range(3):
        loads.append(pltpu.make_async_copy(qkv_hbm.at[s], qkv_ref.at[s], weight_sem.at[2 * s]))
        loads.append(pltpu.make_async_copy(out_hbm.at[s], out_ref.at[s], weight_sem.at[2 * s + 1]))
    loads.append(pltpu.make_async_copy(in_hbm, in_ref, weight_sem.at[6]))
    loads.append(pltpu.make_async_copy(mlp_hbm, mlp_ref, weight_sem.at[7]))
    loads[0].start()
    loads[1].start()

    barrier = pltpu.get_barrier_semaphore()

    @pl.loop(1, devices)
    def _(i):
        other = lax.rem(me + i, devices)
        pl.semaphore_signal(
            barrier, inc=1,
            device_id={"lon": other // lats, "lat": lax.rem(other, lats)},
            device_id_type=pl.DeviceIdType.MESH,
        )

    pl.semaphore_wait(barrier, devices - 1)

    @pl.loop(0, rows)
    def _(r):
        pltpu.make_async_copy(
            x_ref.at[me_lon * rows + r], circ.at[r, me_lon], recv_a.at[r]
        ).start()

        @pl.loop(1, lons)
        def _(i):
            other = lax.rem(me_lon + i, lons)
            pltpu.make_async_remote_copy(
                src_ref=x_ref.at[other * rows + r],
                dst_ref=circ.at[r, me_lon],
                send_sem=send_a,
                recv_sem=recv_a.at[r],
                device_id={"lon": other, "lat": me_lat},
                device_id_type=pl.DeviceIdType.MESH,
            ).start()

    for load in loads[2:]:
        load.start()

    table_ref[...] = jnp.zeros_like(table_ref)
    for start in range(0, table_ref.shape[2], nlon):
        table_ref[0, :, start : start + nlon] = lon_ref[...]
    table_ref[1, :, : 2 * nlat - 1] = lat_ref[...]
    table_ref[2, :, : 2 * lev - 1] = lev_ref[...]
    fill_bias(table_ref, 0, 0, bias_lon, nlon, group_lon)
    fill_bias(table_ref, 1, 1 - nlat, bias_lat, nlat, group_lat)
    fill_bias(table_ref, 2, 1 - lev, bias_lev, lev, LANES)
    loads[0].wait()
    loads[1].wait()

    latitude = me_lat * local_lat + me_lon * rows
    outer = (me_lon < lons // 4) | (me_lon >= lons - lons // 4)
    outer, inner = jnp.logical_not(outer), outer

    def send_meridians(j, first, count, part):
        there = mer.at[j, pl.ds(latitude + first, count)]
        pltpu.make_async_copy(
            outbox.at[j, me, pl.ds(first, count)], there, recv_b.at[j, part]
        ).start()

        @pl.loop(1, devices)
        def _(i):
            other = lax.rem(me + i, devices)
            pltpu.make_async_remote_copy(
                src_ref=outbox.at[j, other, pl.ds(first, count)],
                dst_ref=there,
                send_sem=send_b,
                recv_sem=recv_b.at[j, part],
                device_id={"lon": other // lats, "lat": lax.rem(other, lats)},
                device_id_type=pl.DeviceIdType.MESH,
            ).start()

    def wait_meridians(j, count, part):
        arrived = mer.at[j, pl.ds(0, devices * count)]
        pltpu.make_async_copy(arrived, arrived, recv_b.at[j, part]).wait()

    row_tokens = nlon * lev
    features = gains_ref.shape[1]
    half_slabs = features // LANES // 2
    levels_each = max(1, BLOCK // nlon)

    @pl.loop(0, rows)
    def _(r):
        pltpu.make_async_copy(circ.at[r], circ.at[r], recv_a.at[r]).wait()

        if rows > 1:
            @pl.when(inner & (r == rows - 1))
            def _():
                send_meridians(0, 0, rows - 1, 0)

        arrived = circ[r].astype(F32).reshape(row_tokens, features)
        for c in range(features // LANES):
            lane_row[c] = arrived[:, c * LANES : (c + 1) * LANES]
        for first in range(0, lev, levels_each):
            levels = range(first, first + levels_each)
            state = jnp.concatenate(
                [strided_rows(lane_row, level, nlon, lev) for level in levels], axis=0
            )
            state = sweep_block(
                state, gains_ref[0:1, :], qkv_ref, out_ref, bias_lon, 0, group_lon
            )
            for at, level in enumerate(levels):
                store_strided(lane_row, level, nlon, lev, state[at * nlon : (at + 1) * nlon])
        upper = lax.broadcasted_iota(jnp.int32, (row_tokens, LANES), 0) % (2 * lev) >= lev
        for c in range(half_slabs):
            left, right = lane_row[c], lane_row[c + half_slabs]
            packed = (
                jnp.where(upper, pltpu.roll(right, lev, 0), left),
                jnp.where(upper, right, pltpu.roll(left, row_tokens - lev, 0)),
            )
            for j in range(per_dest):
                outbox[j, :, r, :, c * LANES : (c + 1) * LANES] = (
                    packed[j].reshape(devices, 2 * lev, LANES).astype(BF16)
                )

        if rows > 1:
            @pl.when(outer & (r == rows - 2))
            def _():
                send_meridians(0, 0, rows - 1, 0)

    send_meridians(0, rows - 1, 1, 1)

    @pl.when(outer)
    def _():
        for j in range(1, per_dest):
            send_meridians(j, 0, rows, 0)

    for load in loads[2:]:
        load.wait()

    lat_each = BLOCK // nlat
    half_steps = per_dest * (lats - 1)

    @pl.loop(0, per_dest * lats)
    def _(t):
        j = t // lats
        turn = lax.rem(t, lats)
        target = lax.rem(me_lat + 1 + turn, lats)

        @pl.when(turn == 0)
        def _():
            @pl.when(j == 0)
            def _():
                if rows > 1:
                    wait_meridians(j, rows - 1, 0)
                wait_meridians(j, 1, 1)

            if per_dest > 1:
                @pl.when(j > 0)
                def _():
                    wait_meridians(j, rows, 0)

                @pl.when(inner & (j < per_dest - 1))
                def _():
                    send_meridians(j + 1, 0, rows, 0)

            for c in range(half_slabs):
                lane_mer[c] = (
                    mer[j, :, :, c * LANES : (c + 1) * LANES]
                    .astype(F32)
                    .reshape(nlat * 2 * lev, LANES)
                )

            @pl.loop(0, lev // lat_each)
            def _(b):
                state = jnp.concatenate(
                    [
                        folded_rows(lane_mer, b * lat_each + a, lev, nlat)
                        for a in range(lat_each)
                    ],
                    axis=0,
                )
                state = sweep_block(
                    state, gains_ref[1:2, :], qkv_ref, out_ref, bias_lat, 1, group_lat
                )
                for a in range(lat_each):
                    store_strided(
                        lane_lev, b * lat_each + a, nlat, lev,
                        state[a * nlat : (a + 1) * nlat],
                    )

        start = pl.multiple_of(target * own, own)
        for piece in range(0, own, BLOCK):
            state = jnp.concatenate(
                [
                    lane_lev[c, pl.ds(start + piece, BLOCK), :]
                    for c in range(features // LANES)
                ],
                axis=1,
            )
            state = sweep_block(state, gains_ref[2:3, :], qkv_ref, out_ref, bias_lev, 2, LANES)
            state = feed_forward(state, gains_ref[3:4, :], in_ref, mlp_ref)
            last[t, piece : piece + BLOCK, :] = state.astype(BF16)

        @pl.when(turn < lats - 1)
        def _():
            pltpu.make_async_remote_copy(
                src_ref=last.at[t],
                dst_ref=o_ref.at[me_lat * per_dest + j],
                send_sem=send_c,
                recv_sem=recv_c,
                device_id={"lon": me_lon, "lat": target},
                device_id_type=pl.DeviceIdType.MESH,
            ).start()

        @pl.when(turn == lats - 1)
        def _():
            pltpu.make_async_copy(
                last.at[t], o_ref.at[me_lat * per_dest + j], recv_c
            ).start()

    pltpu.make_async_copy(o_ref, o_ref, recv_c).wait()
    if half_steps:
        sent = last.at[pl.ds(0, half_steps)]
        pltpu.make_async_copy(sent, sent, send_c).wait()

    @pl.loop(0, rows)
    def _(r):
        if lons > 1:
            sent = circ.at[r, pl.ds(0, lons - 1)]
            pltpu.make_async_copy(sent, sent, send_a).wait()

    for j in range(per_dest):
        sent = outbox.at[j, pl.ds(0, devices - 1)]
        pltpu.make_async_copy(sent, sent, send_b).wait()


def per_device(
    lons, lats,
    fields, norm_gains, qkv_weight, out_weight,
    longitude_bias, latitude_bias, level_bias, mlp_in, mlp_out,
):
    local_lat, local_lon, lev, features = fields.shape
    nlon, nlat = local_lon * lons, local_lat * lats
    rows = local_lat // lons
    devices = lons * lats
    per_dest = nlon // devices
    heads = longitude_bias.shape[0]
    hidden = mlp_in.shape[1]
    slabs = features // LANES
    width = max(2 * LANES, 2 * nlat, nlon)
    x = fields.astype(BF16).reshape(local_lat, local_lon * lev, features)
    group_lon, group_lat = max(LANES, nlon), max(LANES, nlat)
    vmem = pl.BlockSpec(memory_space=pltpu.VMEM)
    hbm = pl.BlockSpec(memory_space=pl.ANY)
    own = local_lat * lev
    out = pl.pallas_call(
        functools.partial(kernel, (nlon, nlat, lev, lons, lats, rows, heads)),
        out_shape=jax.ShapeDtypeStruct((local_lon, own, features), BF16),
        in_specs=[hbm, vmem, vmem, vmem, vmem, hbm, hbm, hbm, hbm],
        out_specs=hbm,
        scratch_shapes=[
            pltpu.VMEM(qkv_weight.shape, BF16),
            pltpu.VMEM(out_weight.shape, BF16),
            pltpu.VMEM(mlp_in.shape, BF16),
            pltpu.VMEM(mlp_out.shape, BF16),
            pltpu.VMEM((3, heads, width), F32),
            pltpu.VMEM((heads // 2, group_lon, 2 * group_lon), F32),
            pltpu.VMEM((heads // 2, group_lat, 2 * group_lat), F32),
            pltpu.VMEM((heads // 2, LANES, 2 * LANES), F32),
            pltpu.VMEM((rows, lons, local_lon * lev, features), BF16),
            pltpu.VMEM((per_dest, devices, rows, 2 * lev, features // 2), BF16),
            pltpu.VMEM((per_dest, nlat, 2 * lev, features // 2), BF16),
            pltpu.VMEM((slabs, nlon * lev, LANES), F32),
            pltpu.VMEM((slabs // 2, nlat * 2 * lev, LANES), F32),
            pltpu.VMEM((slabs, nlat * lev, LANES), F32),
            pltpu.VMEM((per_dest * lats, own, features), BF16),
            pltpu.SemaphoreType.DMA((8,)),
            pltpu.SemaphoreType.DMA,
            pltpu.SemaphoreType.DMA((rows,)),
            pltpu.SemaphoreType.DMA,
            pltpu.SemaphoreType.DMA((per_dest, 2)),
            pltpu.SemaphoreType.DMA,
            pltpu.SemaphoreType.DMA,
        ],
        compiler_params=pltpu.CompilerParams(
            collective_id=0, has_side_effects=True, vmem_limit_bytes=64 * 1000 * 1000
        ),
    )(x, norm_gains, longitude_bias, latitude_bias, level_bias, qkv_weight, out_weight, mlp_in, mlp_out)
    out = out.reshape(local_lon, local_lat, lev, features)
    return jnp.swapaxes(out, 0, 1).astype(fields.dtype)


def solution(mesh):
    in_specs = (P("lat", "lon", None, None), P(), P(), P(), P(), P(), P(), P(), P())
    out_specs = P("lat", "lon", None, None)
    return jax.shard_map(
        functools.partial(per_device, mesh.shape["lon"], mesh.shape["lat"]),
        mesh=mesh, in_specs=in_specs, out_specs=out_specs, check_vma=False,
    )
```

```python
import functools

import jax
import jax.numpy as jnp
from jax import lax
from jax.experimental import pallas as pl
from jax.experimental.pallas import tpu as pltpu
from jax.sharding import PartitionSpec as P

HEAD = 64
EPSILON = 1e-06
LANES = 128
BLOCK = 256
NEGATIVE = -1e30
BF16 = jnp.bfloat16
F32 = jnp.float32


def normalize(fields, gain_row):
    square = jnp.mean(fields * fields, axis=-1, keepdims=True)
    return (fields * lax.rsqrt(square + EPSILON) * gain_row).astype(BF16)


def gelu(u):
    inner = u * (0.7978845608028654 + (0.7978845608028654 * 0.044715) * (u * u))
    half = 0.5 * u
    return half + half * jnp.tanh(inner)


def sweep_block(state, gain_row, qkv_ref, out_ref, bias_ref, index, group):
    tokens, features = state.shape
    normed = normalize(state, gain_row)
    qkv = jnp.dot(normed, qkv_ref[index], preferred_element_type=F32).astype(BF16)
    low = lax.broadcasted_iota(jnp.int32, (group, LANES), 1) < HEAD
    zero = jnp.zeros((group, LANES), BF16)
    one = jnp.ones((group, LANES), BF16)
    sums = (jnp.where(low, one, zero), jnp.where(low, zero, one))
    scale = jnp.asarray(HEAD**-0.5, BF16)
    columns = []
    for pair in range(features // LANES):
        rows = []
        for start in range(0, tokens, group):
            here = slice(start, start + group)
            q = qkv[here, pair * LANES : (pair + 1) * LANES] * scale
            k = qkv[here, features + pair * LANES : features + (pair + 1) * LANES]
            v = qkv[here, 2 * features + pair * LANES : 2 * features + (pair + 1) * LANES]
            keys = jnp.concatenate([jnp.where(low, k, zero), jnp.where(low, zero, k)], axis=0)
            scores = lax.dot_general(
                q, keys, (((1,), (1,)), ((), ())), preferred_element_type=F32
            )
            scores = scores + bias_ref[pair]
            halves = []
            for head in range(2):
                part = scores[:, head * group : (head + 1) * group]
                peak = jnp.max(part, axis=-1, keepdims=True)
                halves.append(jnp.exp(part - peak).astype(BF16))
            values = jnp.concatenate(
                [
                    jnp.concatenate([jnp.where(low, v, zero), sums[0]], axis=1),
                    jnp.concatenate([jnp.where(low, zero, v), sums[1]], axis=1),
                ],
                axis=0,
            )
            summed = jnp.dot(
                jnp.concatenate(halves, axis=1), values, preferred_element_type=F32
            )
            rows.append((summed[:, :LANES] / summed[:, LANES:]).astype(BF16))
        columns.append(jnp.concatenate(rows, axis=0))
    attended = jnp.concatenate(columns, axis=1)
    return state + jnp.dot(attended, out_ref[index], preferred_element_type=F32)


def feed_forward(state, gain_row, in_ref, out_ref):
    features = state.shape[1]
    hidden_count = in_ref.shape[1]
    normed = normalize(state, gain_row)
    result = state
    for start in range(0, hidden_count, features):
        u = jnp.dot(normed, in_ref[:, start : start + features], preferred_element_type=F32)
        hidden = gelu(u).astype(BF16)
        result = result + jnp.dot(
            hidden, out_ref[start : start + features, :], preferred_element_type=F32
        )
    return result


def strided_rows(ref, start, count, stride):
    return jnp.concatenate(
        [ref[c, pl.ds(start, count, stride=stride), :] for c in range(ref.shape[0])], axis=1
    )


def folded_rows(ref, row, lev, count):
    return jnp.concatenate(
        [
            ref[c, pl.ds(row + half * lev, count, stride=2 * lev), :]
            for half in range(2)
            for c in range(ref.shape[0])
        ],
        axis=1,
    )


def store_strided(ref, start, count, stride, value):
    for c in range(ref.shape[0]):
        ref[c, pl.ds(start, count, stride=stride), :] = value[:, c * LANES : (c + 1) * LANES]


def fill_bias(table_ref, sweep, shift, bias_ref, length, group):
    heads = 2 * bias_ref.shape[0]
    width = table_ref.shape[2]
    rows = lax.broadcasted_iota(jnp.int32, (group, group), 0) // length
    cols = lax.broadcasted_iota(jnp.int32, (group, group), 1) // length
    for head in range(heads):
        line = jnp.broadcast_to(table_ref[sweep, head : head + 1, :], (group, width))
        line = pltpu.roll(line, shift % width, 1)
        rolled = pltpu.roll(line, 0, 1, stride=1, stride_axis=0)[:, :group]
        if length < group:
            rolled = jnp.where(rows == cols, rolled, NEGATIVE)
        bias_ref[head // 2, :, head % 2 * group : (head % 2 + 1) * group] = rolled


def kernel(
    sizes,
    x_ref, gains_ref, lon_ref, lat_ref, lev_ref, qkv_hbm, out_hbm, in_hbm, mlp_hbm,
    o_ref,
    qkv_ref, out_ref, in_ref, mlp_ref,
    table_ref, bias_lon, bias_lat, bias_lev,
    circ, outbox, mer, lane_row, lane_mer, lane_lev, last,
    weight_sem, send_a, recv_a, send_b, recv_b, send_c, recv_c,
):
    nlon, nlat, lev, lons, lats, rows, heads = sizes
    devices = lons * lats
    me_lon, me_lat = lax.axis_index("lon"), lax.axis_index("lat")
    me = me_lon * lats + me_lat
    local_lat = nlat // lats
    per_dest = nlon // devices
    own = local_lat * lev
    group_lon, group_lat = max(LANES, nlon), max(LANES, nlat)

    loads = []
    for s in range(3):
        loads.append(pltpu.make_async_copy(qkv_hbm.at[s], qkv_ref.at[s], weight_sem.at[2 * s]))
        loads.append(pltpu.make_async_copy(out_hbm.at[s], out_ref.at[s], weight_sem.at[2 * s + 1]))
    loads.append(pltpu.make_async_copy(in_hbm, in_ref, weight_sem.at[6]))
    loads.append(pltpu.make_async_copy(mlp_hbm, mlp_ref, weight_sem.at[7]))
    loads[0].start()
    loads[1].start()

    barrier = pltpu.get_barrier_semaphore()

    @pl.loop(1, devices)
    def _(i):
        other = lax.rem(me + i, devices)
        pl.semaphore_signal(
            barrier, inc=1,
            device_id={"lon": other // lats, "lat": lax.rem(other, lats)},
            device_id_type=pl.DeviceIdType.MESH,
        )

    pl.semaphore_wait(barrier, devices - 1)

    @pl.loop(0, rows)
    def _(r):
        pltpu.make_async_copy(
            x_ref.at[me_lon * rows + r], circ.at[r, me_lon], recv_a.at[r]
        ).start()

        @pl.loop(1, lons)
        def _(i):
            other = lax.rem(me_lon + i, lons)
            pltpu.make_async_remote_copy(
                src_ref=x_ref.at[other * rows + r],
                dst_ref=circ.at[r, me_lon],
                send_sem=send_a,
                recv_sem=recv_a.at[r],
                device_id={"lon": other, "lat": me_lat},
                device_id_type=pl.DeviceIdType.MESH,
            ).start()

    for load in loads[2:]:
        load.start()

    table_ref[...] = jnp.zeros_like(table_ref)
    for start in range(0, table_ref.shape[2], nlon):
        table_ref[0, :, start : start + nlon] = lon_ref[...]
    table_ref[1, :, : 2 * nlat - 1] = lat_ref[...]
    square = bias_lev.at[0, :, :LANES]
    square[...] = jnp.zeros(square.shape, F32)
    square[: 2 * lev - 1, :heads] = lev_ref[...]
    table_ref[2, :, : 2 * lev - 1] = square[...].T[:heads, : 2 * lev - 1]
    fill_bias(table_ref, 0, 0, bias_lon, nlon, group_lon)
    fill_bias(table_ref, 1, 1 - nlat, bias_lat, nlat, group_lat)
    fill_bias(table_ref, 2, 1 - lev, bias_lev, lev, LANES)
    loads[0].wait()
    loads[1].wait()

    latitude = me_lat * local_lat + me_lon * rows
    outer = (me_lon < lons // 4) | (me_lon >= lons - lons // 4)
    outer, inner = jnp.logical_not(outer), outer

    def send_meridians(j, first, count, part):
        there = mer.at[j, pl.ds(latitude + first, count)]
        pltpu.make_async_copy(
            outbox.at[j, me, pl.ds(first, count)], there, recv_b.at[j, part]
        ).start()

        @pl.loop(1, devices)
        def _(i):
            other = lax.rem(me + i, devices)
            pltpu.make_async_remote_copy(
                src_ref=outbox.at[j, other, pl.ds(first, count)],
                dst_ref=there,
                send_sem=send_b,
                recv_sem=recv_b.at[j, part],
                device_id={"lon": other // lats, "lat": lax.rem(other, lats)},
                device_id_type=pl.DeviceIdType.MESH,
            ).start()

    def wait_meridians(j, count, part):
        arrived = mer.at[j, pl.ds(0, devices * count)]
        pltpu.make_async_copy(arrived, arrived, recv_b.at[j, part]).wait()

    row_tokens = nlon * lev
    features = gains_ref.shape[1]
    half_slabs = features // LANES // 2
    levels_each = max(1, BLOCK // nlon)

    @pl.loop(0, rows)
    def _(r):
        pltpu.make_async_copy(circ.at[r], circ.at[r], recv_a.at[r]).wait()

        if rows > 1:
            @pl.when(inner & (r == rows - 1))
            def _():
                send_meridians(0, 0, rows - 1, 0)

        arrived = circ[r].astype(F32).reshape(row_tokens, features)
        for c in range(features // LANES):
            lane_row[c] = arrived[:, c * LANES : (c + 1) * LANES]
        for first in range(0, lev, levels_each):
            levels = range(first, first + levels_each)
            state = jnp.concatenate(
                [strided_rows(lane_row, level, nlon, lev) for level in levels], axis=0
            )
            state = sweep_block(
                state, gains_ref[0:1, :], qkv_ref, out_ref, bias_lon, 0, group_lon
            )
            for at, level in enumerate(levels):
                store_strided(lane_row, level, nlon, lev, state[at * nlon : (at + 1) * nlon])
        upper = lax.broadcasted_iota(jnp.int32, (row_tokens, LANES), 0) % (2 * lev) >= lev
        for c in range(half_slabs):
            left, right = lane_row[c], lane_row[c + half_slabs]
            packed = (
                jnp.where(upper, pltpu.roll(right, lev, 0), left),
                jnp.where(upper, right, pltpu.roll(left, row_tokens - lev, 0)),
            )
            for j in range(per_dest):
                outbox[j, :, r, :, c * LANES : (c + 1) * LANES] = (
                    packed[j].reshape(devices, 2 * lev, LANES).astype(BF16)
                )

        if rows > 1:
            @pl.when(outer & (r == rows - 2))
            def _():
                send_meridians(0, 0, rows - 1, 0)

    send_meridians(0, rows - 1, 1, 1)

    @pl.when(outer)
    def _():
        for j in range(1, per_dest):
            send_meridians(j, 0, rows, 0)

    for load in loads[2:]:
        load.wait()

    lat_each = BLOCK // nlat
    half_steps = per_dest * (lats - 1)

    @pl.loop(0, per_dest * lats)
    def _(t):
        j = t // lats
        turn = lax.rem(t, lats)
        target = lax.rem(me_lat + 1 + turn, lats)

        @pl.when(turn == 0)
        def _():
            @pl.when(j == 0)
            def _():
                if rows > 1:
                    wait_meridians(j, rows - 1, 0)
                wait_meridians(j, 1, 1)

            if per_dest > 1:
                @pl.when(j > 0)
                def _():
                    wait_meridians(j, rows, 0)

                @pl.when(inner & (j < per_dest - 1))
                def _():
                    send_meridians(j + 1, 0, rows, 0)

            for c in range(half_slabs):
                lane_mer[c] = (
                    mer[j, :, :, c * LANES : (c + 1) * LANES]
                    .astype(F32)
                    .reshape(nlat * 2 * lev, LANES)
                )

            @pl.loop(0, lev // lat_each)
            def _(b):
                state = jnp.concatenate(
                    [
                        folded_rows(lane_mer, b * lat_each + a, lev, nlat)
                        for a in range(lat_each)
                    ],
                    axis=0,
                )
                state = sweep_block(
                    state, gains_ref[1:2, :], qkv_ref, out_ref, bias_lat, 1, group_lat
                )
                for a in range(lat_each):
                    store_strided(
                        lane_lev, b * lat_each + a, nlat, lev,
                        state[a * nlat : (a + 1) * nlat],
                    )

        start = pl.multiple_of(target * own, own)
        for piece in range(0, own, BLOCK):
            state = jnp.concatenate(
                [
                    lane_lev[c, pl.ds(start + piece, BLOCK), :]
                    for c in range(features // LANES)
                ],
                axis=1,
            )
            state = sweep_block(state, gains_ref[2:3, :], qkv_ref, out_ref, bias_lev, 2, LANES)
            state = feed_forward(state, gains_ref[3:4, :], in_ref, mlp_ref)
            last[t, piece // lev : (piece + BLOCK) // lev] = (
                state.reshape(BLOCK // lev, lev, features).astype(BF16)
            )

        @pl.when(turn < lats - 1)
        def _():
            pltpu.make_async_remote_copy(
                src_ref=last.at[t],
                dst_ref=o_ref.at[:, me_lat * per_dest + j],
                send_sem=send_c,
                recv_sem=recv_c,
                device_id={"lon": me_lon, "lat": target},
                device_id_type=pl.DeviceIdType.MESH,
            ).start()

        @pl.when(turn == lats - 1)
        def _():
            pltpu.make_async_copy(
                last.at[t], o_ref.at[:, me_lat * per_dest + j], recv_c
            ).start()

    pltpu.make_async_copy(o_ref, o_ref, recv_c).wait()
    if half_steps:
        sent = last.at[pl.ds(0, half_steps)]
        pltpu.make_async_copy(sent, sent, send_c).wait()

    @pl.loop(0, rows)
    def _(r):
        if lons > 1:
            sent = circ.at[r, pl.ds(0, lons - 1)]
            pltpu.make_async_copy(sent, sent, send_a).wait()

    for j in range(per_dest):
        sent = outbox.at[j, pl.ds(0, devices - 1)]
        pltpu.make_async_copy(sent, sent, send_b).wait()


def per_device(
    lons, lats,
    fields, norm_gains, qkv_weight, out_weight,
    longitude_bias, latitude_bias, level_bias, mlp_in, mlp_out,
):
    local_lat, local_lon, lev, features = fields.shape
    nlon, nlat = local_lon * lons, local_lat * lats
    rows = local_lat // lons
    devices = lons * lats
    per_dest = nlon // devices
    heads = longitude_bias.shape[0]
    hidden = mlp_in.shape[1]
    slabs = features // LANES
    width = max(2 * LANES, 2 * nlat, nlon)
    x = fields.astype(BF16)
    group_lon, group_lat = max(LANES, nlon), max(LANES, nlat)
    vmem = pl.BlockSpec(memory_space=pltpu.VMEM)
    hbm = pl.BlockSpec(memory_space=pl.ANY)
    out = pl.pallas_call(
        functools.partial(kernel, (nlon, nlat, lev, lons, lats, rows, heads)),
        out_shape=jax.ShapeDtypeStruct((local_lat, local_lon, lev, features), BF16),
        in_specs=[hbm, vmem, vmem, vmem, vmem, hbm, hbm, hbm, hbm],
        out_specs=hbm,
        scratch_shapes=[
            pltpu.VMEM(qkv_weight.shape, BF16),
            pltpu.VMEM(out_weight.shape, BF16),
            pltpu.VMEM(mlp_in.shape, BF16),
            pltpu.VMEM(mlp_out.shape, BF16),
            pltpu.VMEM((3, heads, width), F32),
            pltpu.VMEM((heads // 2, group_lon, 2 * group_lon), F32),
            pltpu.VMEM((heads // 2, group_lat, 2 * group_lat), F32),
            pltpu.VMEM((heads // 2, LANES, 2 * LANES), F32),
            pltpu.VMEM((rows, lons, local_lon, lev, features), BF16),
            pltpu.VMEM((per_dest, devices, rows, 2 * lev, features // 2), BF16),
            pltpu.VMEM((per_dest, nlat, 2 * lev, features // 2), BF16),
            pltpu.VMEM((slabs, nlon * lev, LANES), F32),
            pltpu.VMEM((slabs // 2, nlat * 2 * lev, LANES), F32),
            pltpu.VMEM((slabs, nlat * lev, LANES), F32),
            pltpu.VMEM((per_dest * lats, local_lat, lev, features), BF16),
            pltpu.SemaphoreType.DMA((8,)),
            pltpu.SemaphoreType.DMA,
            pltpu.SemaphoreType.DMA((rows,)),
            pltpu.SemaphoreType.DMA,
            pltpu.SemaphoreType.DMA((per_dest, 2)),
            pltpu.SemaphoreType.DMA,
            pltpu.SemaphoreType.DMA,
        ],
        compiler_params=pltpu.CompilerParams(
            collective_id=0, has_side_effects=True, vmem_limit_bytes=64 * 1000 * 1000
        ),
    )(x, norm_gains, longitude_bias, latitude_bias, level_bias.T, qkv_weight, out_weight, mlp_in, mlp_out)
    return out.astype(fields.dtype)


def solution(mesh):
    in_specs = (P("lat", "lon", None, None), P(), P(), P(), P(), P(), P(), P(), P())
    out_specs = P("lat", "lon", None, None)
    return jax.shard_map(
        functools.partial(per_device, mesh.shape["lon"], mesh.shape["lat"]),
        mesh=mesh, in_specs=in_specs, out_specs=out_specs, check_vma=False,
    )
```

```python
import functools

import jax
import jax.numpy as jnp
from jax import lax
from jax.experimental import pallas as pl
from jax.experimental.pallas import tpu as pltpu
from jax.sharding import PartitionSpec as P

HEAD = 64
EPSILON = 1e-06
LANES = 128
BLOCK = 256
NEGATIVE = -1e30
BF16 = jnp.bfloat16
F32 = jnp.float32


def normalize(fields, gain_row):
    square = jnp.mean(fields * fields, axis=-1, keepdims=True)
    return (fields * lax.rsqrt(square + EPSILON) * gain_row).astype(BF16)


def gelu(u):
    inner = u * (0.7978845608028654 + (0.7978845608028654 * 0.044715) * (u * u))
    half = 0.5 * u
    return half + half * jnp.tanh(inner)


def sweep_block(state, gain_row, qkv_ref, out_ref, bias_ref, index, group):
    tokens, features = state.shape
    normed = normalize(state, gain_row)
    qkv = jnp.dot(normed, qkv_ref[index], preferred_element_type=F32).astype(BF16)
    low = lax.broadcasted_iota(jnp.int32, (group, LANES), 1) < HEAD
    zero = jnp.zeros((group, LANES), BF16)
    one = jnp.ones((group, LANES), BF16)
    sums = (jnp.where(low, one, zero), jnp.where(low, zero, one))
    scale = jnp.asarray(HEAD**-0.5, BF16)
    columns = []
    for pair in range(features // LANES):
        rows = []
        for start in range(0, tokens, group):
            here = slice(start, start + group)
            q = qkv[here, pair * LANES : (pair + 1) * LANES] * scale
            k = qkv[here, features + pair * LANES : features + (pair + 1) * LANES]
            v = qkv[here, 2 * features + pair * LANES : 2 * features + (pair + 1) * LANES]
            keys = jnp.concatenate([jnp.where(low, k, zero), jnp.where(low, zero, k)], axis=0)
            scores = lax.dot_general(
                q, keys, (((1,), (1,)), ((), ())), preferred_element_type=F32
            )
            scores = scores + bias_ref[pair]
            halves = []
            for head in range(2):
                part = scores[:, head * group : (head + 1) * group]
                peak = jnp.max(part, axis=-1, keepdims=True)
                halves.append(jnp.exp(part - peak).astype(BF16))
            values = jnp.concatenate(
                [
                    jnp.concatenate([jnp.where(low, v, zero), sums[0]], axis=1),
                    jnp.concatenate([jnp.where(low, zero, v), sums[1]], axis=1),
                ],
                axis=0,
            )
            summed = jnp.dot(
                jnp.concatenate(halves, axis=1), values, preferred_element_type=F32
            )
            rows.append((summed[:, :LANES] / summed[:, LANES:]).astype(BF16))
        columns.append(jnp.concatenate(rows, axis=0))
    attended = jnp.concatenate(columns, axis=1)
    return state + jnp.dot(attended, out_ref[index], preferred_element_type=F32)


def feed_forward(state, gain_row, in_ref, out_ref):
    features = state.shape[1]
    hidden_count = in_ref.shape[1]
    normed = normalize(state, gain_row)
    result = state
    for start in range(0, hidden_count, features):
        u = jnp.dot(normed, in_ref[:, start : start + features], preferred_element_type=F32)
        hidden = gelu(u).astype(BF16)
        result = result + jnp.dot(
            hidden, out_ref[start : start + features, :], preferred_element_type=F32
        )
    return result


def strided_rows(ref, start, count, stride):
    return jnp.concatenate(
        [ref[c, pl.ds(start, count, stride=stride), :] for c in range(ref.shape[0])], axis=1
    )


def folded_rows(ref, row, lev, count):
    return jnp.concatenate(
        [
            ref[c, pl.ds(row + half * lev, count, stride=2 * lev), :]
            for half in range(2)
            for c in range(ref.shape[0])
        ],
        axis=1,
    )


def store_strided(ref, start, count, stride, value):
    for c in range(ref.shape[0]):
        ref[c, pl.ds(start, count, stride=stride), :] = value[:, c * LANES : (c + 1) * LANES]


def fill_bias(table_ref, sweep, shift, bias_ref, length, group):
    heads = 2 * bias_ref.shape[0]
    width = table_ref.shape[2]
    rows = lax.broadcasted_iota(jnp.int32, (group, group), 0) // length
    cols = lax.broadcasted_iota(jnp.int32, (group, group), 1) // length
    for head in range(heads):
        line = jnp.broadcast_to(table_ref[sweep, head : head + 1, :], (group, width))
        line = pltpu.roll(line, shift % width, 1)
        rolled = pltpu.roll(line, 0, 1, stride=1, stride_axis=0)[:, :group]
        if length < group:
            rolled = jnp.where(rows == cols, rolled, NEGATIVE)
        bias_ref[head // 2, :, head % 2 * group : (head % 2 + 1) * group] = rolled


def kernel(
    sizes,
    x_ref, gains_ref, lon_ref, lat_ref, lev_ref, qkv_hbm, out_hbm, in_hbm, mlp_hbm,
    o_ref,
    qkv_ref, out_ref, in_ref, mlp_ref,
    table_ref, bias_lon, bias_lat, bias_lev,
    wide, narrow, circ, outbox, mer, lane_row, lane_mer, lane_lev, last,
    fields_sem, weight_sem, send_a, recv_a, send_b, recv_b, send_c, recv_c,
):
    nlon, nlat, lev, lons, lats, rows, heads = sizes
    devices = lons * lats
    me_lon, me_lat = lax.axis_index("lon"), lax.axis_index("lat")
    me = me_lon * lats + me_lat
    local_lat = nlat // lats
    per_dest = nlon // devices
    own = local_lat * lev
    group_lon, group_lat = max(LANES, nlon), max(LANES, nlat)

    loads = []
    for s in range(3):
        loads.append(pltpu.make_async_copy(qkv_hbm.at[s], qkv_ref.at[s], weight_sem.at[2 * s]))
        loads.append(pltpu.make_async_copy(out_hbm.at[s], out_ref.at[s], weight_sem.at[2 * s + 1]))
    loads.append(pltpu.make_async_copy(in_hbm, in_ref, weight_sem.at[6]))
    loads.append(pltpu.make_async_copy(mlp_hbm, mlp_ref, weight_sem.at[7]))
    fields_in = [
        pltpu.make_async_copy(x_ref.at[:, r], wide.at[r], fields_sem.at[r]) for r in range(rows)
    ]
    for load in fields_in + loads[:2]:
        load.start()

    barrier = pltpu.get_barrier_semaphore()

    @pl.loop(1, devices)
    def _(i):
        other = lax.rem(me + i, devices)
        pl.semaphore_signal(
            barrier, inc=1,
            device_id={"lon": other // lats, "lat": lax.rem(other, lats)},
            device_id_type=pl.DeviceIdType.MESH,
        )

    pl.semaphore_wait(barrier, devices - 1)

    @pl.loop(0, rows)
    def _(r):
        pltpu.make_async_copy(x_ref.at[:, r], wide.at[r], fields_sem.at[r]).wait()
        narrow[r] = wide[r].astype(BF16)
        pltpu.make_async_copy(
            narrow.at[r, me_lon], circ.at[r, me_lon], recv_a.at[r]
        ).start()

        @pl.loop(1, lons)
        def _(i):
            other = lax.rem(me_lon + i, lons)
            pltpu.make_async_remote_copy(
                src_ref=narrow.at[r, other],
                dst_ref=circ.at[r, me_lon],
                send_sem=send_a,
                recv_sem=recv_a.at[r],
                device_id={"lon": other, "lat": me_lat},
                device_id_type=pl.DeviceIdType.MESH,
            ).start()

    for load in loads[2:]:
        load.start()

    table_ref[...] = jnp.zeros_like(table_ref)
    for start in range(0, table_ref.shape[2], nlon):
        table_ref[0, :, start : start + nlon] = lon_ref[...]
    table_ref[1, :, : 2 * nlat - 1] = lat_ref[...]
    square = bias_lev.at[0, :, :LANES]
    square[...] = jnp.zeros(square.shape, F32)
    square[: 2 * lev - 1, :heads] = lev_ref[...]
    table_ref[2, :, : 2 * lev - 1] = square[...].T[:heads, : 2 * lev - 1]
    fill_bias(table_ref, 0, 0, bias_lon, nlon, group_lon)
    fill_bias(table_ref, 1, 1 - nlat, bias_lat, nlat, group_lat)
    fill_bias(table_ref, 2, 1 - lev, bias_lev, lev, LANES)
    loads[0].wait()
    loads[1].wait()

    latitude = me_lat * local_lat + me_lon * rows
    outer = (me_lon < lons // 4) | (me_lon >= lons - lons // 4)
    outer, inner = jnp.logical_not(outer), outer

    def send_meridians(j, first, count, part):
        there = mer.at[j, pl.ds(latitude + first, count)]
        pltpu.make_async_copy(
            outbox.at[j, me, pl.ds(first, count)], there, recv_b.at[j, part]
        ).start()

        @pl.loop(1, devices)
        def _(i):
            other = lax.rem(me + i, devices)
            pltpu.make_async_remote_copy(
                src_ref=outbox.at[j, other, pl.ds(first, count)],
                dst_ref=there,
                send_sem=send_b,
                recv_sem=recv_b.at[j, part],
                device_id={"lon": other // lats, "lat": lax.rem(other, lats)},
                device_id_type=pl.DeviceIdType.MESH,
            ).start()

    def wait_meridians(j, count, part):
        arrived = mer.at[j, pl.ds(0, devices * count)]
        pltpu.make_async_copy(arrived, arrived, recv_b.at[j, part]).wait()

    row_tokens = nlon * lev
    features = gains_ref.shape[1]
    half_slabs = features // LANES // 2
    levels_each = max(1, BLOCK // nlon)

    @pl.loop(0, rows)
    def _(r):
        pltpu.make_async_copy(circ.at[r], circ.at[r], recv_a.at[r]).wait()

        if rows > 1:
            @pl.when(inner & (r == rows - 1))
            def _():
                send_meridians(0, 0, rows - 1, 0)

        arrived = circ[r].astype(F32).reshape(row_tokens, features)
        for c in range(features // LANES):
            lane_row[c] = arrived[:, c * LANES : (c + 1) * LANES]
        for first in range(0, lev, levels_each):
            levels = range(first, first + levels_each)
            state = jnp.concatenate(
                [strided_rows(lane_row, level, nlon, lev) for level in levels], axis=0
            )
            state = sweep_block(
                state, gains_ref[0:1, :], qkv_ref, out_ref, bias_lon, 0, group_lon
            )
            for at, level in enumerate(levels):
                store_strided(lane_row, level, nlon, lev, state[at * nlon : (at + 1) * nlon])
        upper = lax.broadcasted_iota(jnp.int32, (row_tokens, LANES), 0) % (2 * lev) >= lev
        for c in range(half_slabs):
            left, right = lane_row[c], lane_row[c + half_slabs]
            packed = (
                jnp.where(upper, pltpu.roll(right, lev, 0), left),
                jnp.where(upper, right, pltpu.roll(left, row_tokens - lev, 0)),
            )
            for j in range(per_dest):
                outbox[j, :, r, :, c * LANES : (c + 1) * LANES] = (
                    packed[j].reshape(devices, 2 * lev, LANES).astype(BF16)
                )

        if rows > 1:
            @pl.when(outer & (r == rows - 2))
            def _():
                send_meridians(0, 0, rows - 1, 0)

    send_meridians(0, rows - 1, 1, 1)

    @pl.when(outer)
    def _():
        for j in range(1, per_dest):
            send_meridians(j, 0, rows, 0)

    for load in loads[2:]:
        load.wait()

    lat_each = BLOCK // nlat
    half_steps = per_dest * (lats - 1)

    @pl.loop(0, per_dest * lats)
    def _(t):
        j = t // lats
        turn = lax.rem(t, lats)
        target = lax.rem(me_lat + 1 + turn, lats)

        @pl.when(turn == 0)
        def _():
            @pl.when(j == 0)
            def _():
                if rows > 1:
                    wait_meridians(j, rows - 1, 0)
                wait_meridians(j, 1, 1)

            if per_dest > 1:
                @pl.when(j > 0)
                def _():
                    wait_meridians(j, rows, 0)

                @pl.when(inner & (j < per_dest - 1))
                def _():
                    send_meridians(j + 1, 0, rows, 0)

            for c in range(half_slabs):
                lane_mer[c] = (
                    mer[j, :, :, c * LANES : (c + 1) * LANES]
                    .astype(F32)
                    .reshape(nlat * 2 * lev, LANES)
                )

            @pl.loop(0, lev // lat_each)
            def _(b):
                state = jnp.concatenate(
                    [
                        folded_rows(lane_mer, b * lat_each + a, lev, nlat)
                        for a in range(lat_each)
                    ],
                    axis=0,
                )
                state = sweep_block(
                    state, gains_ref[1:2, :], qkv_ref, out_ref, bias_lat, 1, group_lat
                )
                for a in range(lat_each):
                    store_strided(
                        lane_lev, b * lat_each + a, nlat, lev,
                        state[a * nlat : (a + 1) * nlat],
                    )

        start = pl.multiple_of(target * own, own)
        for piece in range(0, own, BLOCK):
            state = jnp.concatenate(
                [
                    lane_lev[c, pl.ds(start + piece, BLOCK), :]
                    for c in range(features // LANES)
                ],
                axis=1,
            )
            state = sweep_block(state, gains_ref[2:3, :], qkv_ref, out_ref, bias_lev, 2, LANES)
            state = feed_forward(state, gains_ref[3:4, :], in_ref, mlp_ref)
            last[t, piece // lev : (piece + BLOCK) // lev] = (
                state.reshape(BLOCK // lev, lev, features).astype(BF16)
            )

        @pl.when(turn < lats - 1)
        def _():
            pltpu.make_async_remote_copy(
                src_ref=last.at[t],
                dst_ref=o_ref.at[:, me_lat * per_dest + j],
                send_sem=send_c,
                recv_sem=recv_c,
                device_id={"lon": me_lon, "lat": target},
                device_id_type=pl.DeviceIdType.MESH,
            ).start()

        @pl.when(turn == lats - 1)
        def _():
            pltpu.make_async_copy(
                last.at[t], o_ref.at[:, me_lat * per_dest + j], recv_c
            ).start()

    pltpu.make_async_copy(o_ref, o_ref, recv_c).wait()
    if half_steps:
        sent = last.at[pl.ds(0, half_steps)]
        pltpu.make_async_copy(sent, sent, send_c).wait()

    @pl.loop(0, rows)
    def _(r):
        if lons > 1:
            sent = circ.at[r, pl.ds(0, lons - 1)]
            pltpu.make_async_copy(sent, sent, send_a).wait()

    for j in range(per_dest):
        sent = outbox.at[j, pl.ds(0, devices - 1)]
        pltpu.make_async_copy(sent, sent, send_b).wait()


def per_device(
    lons, lats,
    fields, norm_gains, qkv_weight, out_weight,
    longitude_bias, latitude_bias, level_bias, mlp_in, mlp_out,
):
    local_lat, local_lon, lev, features = fields.shape
    nlon, nlat = local_lon * lons, local_lat * lats
    rows = local_lat // lons
    devices = lons * lats
    per_dest = nlon // devices
    heads = longitude_bias.shape[0]
    hidden = mlp_in.shape[1]
    slabs = features // LANES
    width = max(2 * LANES, 2 * nlat, nlon)
    x = fields.reshape(lons, rows, local_lon, lev, features)
    group_lon, group_lat = max(LANES, nlon), max(LANES, nlat)
    vmem = pl.BlockSpec(memory_space=pltpu.VMEM)
    hbm = pl.BlockSpec(memory_space=pl.ANY)
    out = pl.pallas_call(
        functools.partial(kernel, (nlon, nlat, lev, lons, lats, rows, heads)),
        out_shape=jax.ShapeDtypeStruct((local_lat, local_lon, lev, features), BF16),
        in_specs=[hbm, vmem, vmem, vmem, vmem, hbm, hbm, hbm, hbm],
        out_specs=hbm,
        scratch_shapes=[
            pltpu.VMEM(qkv_weight.shape, BF16),
            pltpu.VMEM(out_weight.shape, BF16),
            pltpu.VMEM(mlp_in.shape, BF16),
            pltpu.VMEM(mlp_out.shape, BF16),
            pltpu.VMEM((3, heads, width), F32),
            pltpu.VMEM((heads // 2, group_lon, 2 * group_lon), F32),
            pltpu.VMEM((heads // 2, group_lat, 2 * group_lat), F32),
            pltpu.VMEM((heads // 2, LANES, 2 * LANES), F32),
            pltpu.VMEM((rows, lons, local_lon, lev, features), F32),
            pltpu.VMEM((rows, lons, local_lon, lev, features), BF16),
            pltpu.VMEM((rows, lons, local_lon, lev, features), BF16),
            pltpu.VMEM((per_dest, devices, rows, 2 * lev, features // 2), BF16),
            pltpu.VMEM((per_dest, nlat, 2 * lev, features // 2), BF16),
            pltpu.VMEM((slabs, nlon * lev, LANES), F32),
            pltpu.VMEM((slabs // 2, nlat * 2 * lev, LANES), F32),
            pltpu.VMEM((slabs, nlat * lev, LANES), F32),
            pltpu.VMEM((per_dest * lats, local_lat, lev, features), BF16),
            pltpu.SemaphoreType.DMA((rows,)),
            pltpu.SemaphoreType.DMA((8,)),
            pltpu.SemaphoreType.DMA,
            pltpu.SemaphoreType.DMA((rows,)),
            pltpu.SemaphoreType.DMA,
            pltpu.SemaphoreType.DMA((per_dest, 2)),
            pltpu.SemaphoreType.DMA,
            pltpu.SemaphoreType.DMA,
        ],
        compiler_params=pltpu.CompilerParams(
            collective_id=0, has_side_effects=True, vmem_limit_bytes=64 * 1000 * 1000
        ),
    )(x, norm_gains, longitude_bias, latitude_bias, level_bias.T, qkv_weight, out_weight, mlp_in, mlp_out)
    return out.astype(fields.dtype)


def solution(mesh):
    in_specs = (P("lat", "lon", None, None), P(), P(), P(), P(), P(), P(), P(), P())
    out_specs = P("lat", "lon", None, None)
    return jax.shard_map(
        functools.partial(per_device, mesh.shape["lon"], mesh.shape["lat"]),
        mesh=mesh, in_specs=in_specs, out_specs=out_specs, check_vma=False,
    )
```

```python
import functools

import jax
import jax.numpy as jnp
from jax import lax
from jax.experimental import pallas as pl
from jax.experimental.pallas import tpu as pltpu
from jax.sharding import PartitionSpec as P

HEAD = 64
EPSILON = 1e-06
LANES = 128
BLOCK = 256
NEGATIVE = -1e30
BF16 = jnp.bfloat16
F32 = jnp.float32


def normalize(fields, gain_row):
    square = jnp.mean(fields * fields, axis=-1, keepdims=True)
    return (fields * lax.rsqrt(square + EPSILON) * gain_row).astype(BF16)


def gelu(u):
    inner = u * (0.7978845608028654 + (0.7978845608028654 * 0.044715) * (u * u))
    half = 0.5 * u
    return half + half * jnp.tanh(inner)


def sweep_block(state, gain_row, qkv_ref, out_ref, bias_ref, index, group):
    tokens, features = state.shape
    normed = normalize(state, gain_row)
    qkv = jnp.dot(normed, qkv_ref[index], preferred_element_type=F32).astype(BF16)
    low = lax.broadcasted_iota(jnp.int32, (group, LANES), 1) < HEAD
    zero = jnp.zeros((group, LANES), BF16)
    one = jnp.ones((group, LANES), BF16)
    sums = (jnp.where(low, one, zero), jnp.where(low, zero, one))
    scale = jnp.asarray(HEAD**-0.5, BF16)
    columns = []
    for pair in range(features // LANES):
        rows = []
        for start in range(0, tokens, group):
            here = slice(start, start + group)
            q = qkv[here, pair * LANES : (pair + 1) * LANES] * scale
            k = qkv[here, features + pair * LANES : features + (pair + 1) * LANES]
            v = qkv[here, 2 * features + pair * LANES : 2 * features + (pair + 1) * LANES]
            keys = jnp.concatenate([jnp.where(low, k, zero), jnp.where(low, zero, k)], axis=0)
            scores = lax.dot_general(
                q, keys, (((1,), (1,)), ((), ())), preferred_element_type=F32
            )
            scores = scores + bias_ref[pair]
            halves = []
            for head in range(2):
                part = scores[:, head * group : (head + 1) * group]
                peak = jnp.max(part, axis=-1, keepdims=True)
                halves.append(jnp.exp(part - peak).astype(BF16))
            values = jnp.concatenate(
                [
                    jnp.concatenate([jnp.where(low, v, zero), sums[0]], axis=1),
                    jnp.concatenate([jnp.where(low, zero, v), sums[1]], axis=1),
                ],
                axis=0,
            )
            summed = jnp.dot(
                jnp.concatenate(halves, axis=1), values, preferred_element_type=F32
            )
            rows.append((summed[:, :LANES] / summed[:, LANES:]).astype(BF16))
        columns.append(jnp.concatenate(rows, axis=0))
    attended = jnp.concatenate(columns, axis=1)
    return state + jnp.dot(attended, out_ref[index], preferred_element_type=F32)


def feed_forward(state, gain_row, in_ref, out_ref):
    features = state.shape[1]
    hidden_count = in_ref.shape[1]
    normed = normalize(state, gain_row)
    result = state
    for start in range(0, hidden_count, features):
        u = jnp.dot(normed, in_ref[:, start : start + features], preferred_element_type=F32)
        hidden = gelu(u).astype(BF16)
        result = result + jnp.dot(
            hidden, out_ref[start : start + features, :], preferred_element_type=F32
        )
    return result


def strided_rows(ref, start, count, stride):
    return jnp.concatenate(
        [ref[c, pl.ds(start, count, stride=stride), :] for c in range(ref.shape[0])], axis=1
    )


def folded_rows(ref, row, lev, count):
    return jnp.concatenate(
        [
            ref[c, pl.ds(row + half * lev, count, stride=2 * lev), :]
            for half in range(2)
            for c in range(ref.shape[0])
        ],
        axis=1,
    )


def store_strided(ref, start, count, stride, value):
    for c in range(ref.shape[0]):
        ref[c, pl.ds(start, count, stride=stride), :] = value[:, c * LANES : (c + 1) * LANES]


def fill_bias(table_ref, sweep, shift, bias_ref, length, group):
    heads = 2 * bias_ref.shape[0]
    width = table_ref.shape[2]
    rows = lax.broadcasted_iota(jnp.int32, (group, group), 0) // length
    cols = lax.broadcasted_iota(jnp.int32, (group, group), 1) // length
    for head in range(heads):
        line = jnp.broadcast_to(table_ref[sweep, head : head + 1, :], (group, width))
        line = pltpu.roll(line, shift % width, 1)
        rolled = pltpu.roll(line, 0, 1, stride=1, stride_axis=0)[:, :group]
        if length < group:
            rolled = jnp.where(rows == cols, rolled, NEGATIVE)
        bias_ref[head // 2, :, head % 2 * group : (head % 2 + 1) * group] = rolled


def kernel(
    sizes,
    x_ref, gains_ref, lon_ref, lat_ref, lev_ref, qkv_hbm, out_hbm, in_hbm, mlp_hbm,
    o_ref,
    qkv_ref, out_ref, in_ref, mlp_ref,
    table_ref, bias_lon, bias_lat, bias_lev,
    wide, narrow, circ, outbox, mer, lane_row, lane_mer, lane_lev, last,
    fields_sem, weight_sem, send_a, recv_a, send_b, recv_b, send_c, recv_c,
):
    nlon, nlat, lev, lons, lats, rows, heads = sizes
    devices = lons * lats
    me_lon, me_lat = lax.axis_index("lon"), lax.axis_index("lat")
    me = me_lon * lats + me_lat
    local_lat = nlat // lats
    per_dest = nlon // devices
    own = local_lat * lev
    group_lon, group_lat = max(LANES, nlon), max(LANES, nlat)

    loads = []
    for s in range(3):
        loads.append(pltpu.make_async_copy(qkv_hbm.at[s], qkv_ref.at[s], weight_sem.at[2 * s]))
        loads.append(pltpu.make_async_copy(out_hbm.at[s], out_ref.at[s], weight_sem.at[2 * s + 1]))
    loads.append(pltpu.make_async_copy(in_hbm, in_ref, weight_sem.at[6]))
    loads.append(pltpu.make_async_copy(mlp_hbm, mlp_ref, weight_sem.at[7]))
    fields_in = [
        pltpu.make_async_copy(x_ref.at[:, r], wide.at[r], fields_sem.at[r]) for r in range(rows)
    ]
    for load in fields_in + loads[:2]:
        load.start()

    barrier = pltpu.get_barrier_semaphore()

    @pl.loop(1, devices)
    def _(i):
        other = lax.rem(me + i, devices)
        pl.semaphore_signal(
            barrier, inc=1,
            device_id={"lon": other // lats, "lat": lax.rem(other, lats)},
            device_id_type=pl.DeviceIdType.MESH,
        )

    pl.semaphore_wait(barrier, devices - 1)

    @pl.loop(0, rows)
    def _(r):
        pltpu.make_async_copy(x_ref.at[:, r], wide.at[r], fields_sem.at[r]).wait()
        narrow[r] = wide[r].astype(BF16)
        pltpu.make_async_copy(
            narrow.at[r, me_lon], circ.at[r, me_lon], recv_a.at[r]
        ).start()

        @pl.loop(1, lons)
        def _(i):
            other = lax.rem(me_lon + i, lons)
            pltpu.make_async_remote_copy(
                src_ref=narrow.at[r, other],
                dst_ref=circ.at[r, me_lon],
                send_sem=send_a,
                recv_sem=recv_a.at[r],
                device_id={"lon": other, "lat": me_lat},
                device_id_type=pl.DeviceIdType.MESH,
            ).start()

    for load in loads[2:]:
        load.start()

    table_ref[...] = jnp.zeros_like(table_ref)
    for start in range(0, table_ref.shape[2], nlon):
        table_ref[0, :, start : start + nlon] = lon_ref[...]
    table_ref[1, :, : 2 * nlat - 1] = lat_ref[...]
    square = bias_lev.at[0, :, :LANES]
    square[...] = jnp.zeros(square.shape, F32)
    square[: 2 * lev - 1, :heads] = lev_ref[...]
    table_ref[2, :, : 2 * lev - 1] = square[...].T[:heads, : 2 * lev - 1]
    fill_bias(table_ref, 0, 0, bias_lon, nlon, group_lon)
    fill_bias(table_ref, 1, 1 - nlat, bias_lat, nlat, group_lat)
    fill_bias(table_ref, 2, 1 - lev, bias_lev, lev, LANES)
    loads[0].wait()
    loads[1].wait()

    latitude = me_lat * local_lat + me_lon * rows
    outer = (me_lon < lons // 4) | (me_lon >= lons - lons // 4)
    outer, inner = jnp.logical_not(outer), outer

    def send_meridians(j, first, count, part):
        there = mer.at[j, pl.ds(latitude + first, count)]
        pltpu.make_async_copy(
            outbox.at[j, me, pl.ds(first, count)], there, recv_b.at[j, part]
        ).start()

        @pl.loop(1, devices)
        def _(i):
            other = lax.rem(me + i, devices)
            pltpu.make_async_remote_copy(
                src_ref=outbox.at[j, other, pl.ds(first, count)],
                dst_ref=there,
                send_sem=send_b,
                recv_sem=recv_b.at[j, part],
                device_id={"lon": other // lats, "lat": lax.rem(other, lats)},
                device_id_type=pl.DeviceIdType.MESH,
            ).start()

    def wait_meridians(j, count, part):
        arrived = mer.at[j, pl.ds(0, devices * count)]
        pltpu.make_async_copy(arrived, arrived, recv_b.at[j, part]).wait()

    row_tokens = nlon * lev
    features = gains_ref.shape[1]
    half_slabs = features // LANES // 2
    levels_each = max(1, BLOCK // nlon)

    @pl.loop(0, rows)
    def _(r):
        pltpu.make_async_copy(circ.at[r], circ.at[r], recv_a.at[r]).wait()

        if rows > 1:
            @pl.when(inner & (r == rows - 1))
            def _():
                send_meridians(0, 0, rows - 1, 0)

        arrived = circ[r].astype(F32).reshape(row_tokens, features)
        for c in range(features // LANES):
            lane_row[c] = arrived[:, c * LANES : (c + 1) * LANES]
        for first in range(0, lev, levels_each):
            levels = range(first, first + levels_each)
            state = jnp.concatenate(
                [strided_rows(lane_row, level, nlon, lev) for level in levels], axis=0
            )
            state = sweep_block(
                state, gains_ref[0:1, :], qkv_ref, out_ref, bias_lon, 0, group_lon
            )
            for at, level in enumerate(levels):
                store_strided(lane_row, level, nlon, lev, state[at * nlon : (at + 1) * nlon])
        upper = lax.broadcasted_iota(jnp.int32, (row_tokens, LANES), 0) % (2 * lev) >= lev
        for c in range(half_slabs):
            left, right = lane_row[c], lane_row[c + half_slabs]
            packed = (
                jnp.where(upper, pltpu.roll(right, lev, 0), left),
                jnp.where(upper, right, pltpu.roll(left, row_tokens - lev, 0)),
            )
            for j in range(per_dest):
                outbox[j, :, r, :, c * LANES : (c + 1) * LANES] = (
                    packed[j].reshape(devices, 2 * lev, LANES).astype(BF16)
                )

        if rows > 1:
            @pl.when(outer & (r == rows - 2))
            def _():
                send_meridians(0, 0, rows - 1, 0)

    send_meridians(0, rows - 1, 1, 1)

    @pl.when(outer)
    def _():
        for j in range(1, per_dest):
            send_meridians(j, 0, rows, 0)

    for load in loads[2:]:
        load.wait()

    lat_each = BLOCK // nlat
    half_steps = per_dest * (lats - 1)

    @pl.loop(0, per_dest * lats)
    def _(t):
        j = t // lats
        turn = lax.rem(t, lats)
        target = lax.rem(me_lat + 1 + turn, lats)

        @pl.when(turn == 0)
        def _():
            @pl.when(j == 0)
            def _():
                if rows > 1:
                    wait_meridians(j, rows - 1, 0)
                if per_dest > 1:
                    @pl.when(inner)
                    def _():
                        send_meridians(1, 0, rows, 0)

                wait_meridians(j, 1, 1)

            if per_dest > 1:
                @pl.when(j > 0)
                def _():
                    wait_meridians(j, rows, 0)

                @pl.when(inner & (j > 0) & (j < per_dest - 1))
                def _():
                    send_meridians(j + 1, 0, rows, 0)

            for c in range(half_slabs):
                lane_mer[c] = (
                    mer[j, :, :, c * LANES : (c + 1) * LANES]
                    .astype(F32)
                    .reshape(nlat * 2 * lev, LANES)
                )

            @pl.loop(0, lev // lat_each)
            def _(b):
                state = jnp.concatenate(
                    [
                        folded_rows(lane_mer, b * lat_each + a, lev, nlat)
                        for a in range(lat_each)
                    ],
                    axis=0,
                )
                state = sweep_block(
                    state, gains_ref[1:2, :], qkv_ref, out_ref, bias_lat, 1, group_lat
                )
                for a in range(lat_each):
                    store_strided(
                        lane_lev, b * lat_each + a, nlat, lev,
                        state[a * nlat : (a + 1) * nlat],
                    )

        start = pl.multiple_of(target * own, own)
        for piece in range(0, own, BLOCK):
            state = jnp.concatenate(
                [
                    lane_lev[c, pl.ds(start + piece, BLOCK), :]
                    for c in range(features // LANES)
                ],
                axis=1,
            )
            state = sweep_block(state, gains_ref[2:3, :], qkv_ref, out_ref, bias_lev, 2, LANES)
            state = feed_forward(state, gains_ref[3:4, :], in_ref, mlp_ref)
            last[t, piece // lev : (piece + BLOCK) // lev] = (
                state.reshape(BLOCK // lev, lev, features).astype(BF16)
            )

        @pl.when(turn < lats - 1)
        def _():
            pltpu.make_async_remote_copy(
                src_ref=last.at[t],
                dst_ref=o_ref.at[:, me_lat * per_dest + j],
                send_sem=send_c,
                recv_sem=recv_c,
                device_id={"lon": me_lon, "lat": target},
                device_id_type=pl.DeviceIdType.MESH,
            ).start()

        @pl.when(turn == lats - 1)
        def _():
            pltpu.make_async_copy(
                last.at[t], o_ref.at[:, me_lat * per_dest + j], recv_c
            ).start()

    pltpu.make_async_copy(o_ref, o_ref, recv_c).wait()
    if half_steps:
        sent = last.at[pl.ds(0, half_steps)]
        pltpu.make_async_copy(sent, sent, send_c).wait()

    @pl.loop(0, rows)
    def _(r):
        if lons > 1:
            sent = circ.at[r, pl.ds(0, lons - 1)]
            pltpu.make_async_copy(sent, sent, send_a).wait()

    for j in range(per_dest):
        sent = outbox.at[j, pl.ds(0, devices - 1)]
        pltpu.make_async_copy(sent, sent, send_b).wait()


def per_device(
    lons, lats,
    fields, norm_gains, qkv_weight, out_weight,
    longitude_bias, latitude_bias, level_bias, mlp_in, mlp_out,
):
    local_lat, local_lon, lev, features = fields.shape
    nlon, nlat = local_lon * lons, local_lat * lats
    rows = local_lat // lons
    devices = lons * lats
    per_dest = nlon // devices
    heads = longitude_bias.shape[0]
    hidden = mlp_in.shape[1]
    slabs = features // LANES
    width = max(2 * LANES, 2 * nlat, nlon)
    x = fields.reshape(lons, rows, local_lon, lev, features)
    group_lon, group_lat = max(LANES, nlon), max(LANES, nlat)
    vmem = pl.BlockSpec(memory_space=pltpu.VMEM)
    hbm = pl.BlockSpec(memory_space=pl.ANY)
    out = pl.pallas_call(
        functools.partial(kernel, (nlon, nlat, lev, lons, lats, rows, heads)),
        out_shape=jax.ShapeDtypeStruct((local_lat, local_lon, lev, features), BF16),
        in_specs=[hbm, vmem, vmem, vmem, vmem, hbm, hbm, hbm, hbm],
        out_specs=hbm,
        scratch_shapes=[
            pltpu.VMEM(qkv_weight.shape, BF16),
            pltpu.VMEM(out_weight.shape, BF16),
            pltpu.VMEM(mlp_in.shape, BF16),
            pltpu.VMEM(mlp_out.shape, BF16),
            pltpu.VMEM((3, heads, width), F32),
            pltpu.VMEM((heads // 2, group_lon, 2 * group_lon), F32),
            pltpu.VMEM((heads // 2, group_lat, 2 * group_lat), F32),
            pltpu.VMEM((heads // 2, LANES, 2 * LANES), F32),
            pltpu.VMEM((rows, lons, local_lon, lev, features), F32),
            pltpu.VMEM((rows, lons, local_lon, lev, features), BF16),
            pltpu.VMEM((rows, lons, local_lon, lev, features), BF16),
            pltpu.VMEM((per_dest, devices, rows, 2 * lev, features // 2), BF16),
            pltpu.VMEM((per_dest, nlat, 2 * lev, features // 2), BF16),
            pltpu.VMEM((slabs, nlon * lev, LANES), F32),
            pltpu.VMEM((slabs // 2, nlat * 2 * lev, LANES), F32),
            pltpu.VMEM((slabs, nlat * lev, LANES), F32),
            pltpu.VMEM((per_dest * lats, local_lat, lev, features), BF16),
            pltpu.SemaphoreType.DMA((rows,)),
            pltpu.SemaphoreType.DMA((8,)),
            pltpu.SemaphoreType.DMA,
            pltpu.SemaphoreType.DMA((rows,)),
            pltpu.SemaphoreType.DMA,
            pltpu.SemaphoreType.DMA((per_dest, 2)),
            pltpu.SemaphoreType.DMA,
            pltpu.SemaphoreType.DMA,
        ],
        compiler_params=pltpu.CompilerParams(
            collective_id=0, has_side_effects=True, vmem_limit_bytes=64 * 1000 * 1000
        ),
    )(x, norm_gains, longitude_bias, latitude_bias, level_bias.T, qkv_weight, out_weight, mlp_in, mlp_out)
    return out.astype(fields.dtype)


def solution(mesh):
    in_specs = (P("lat", "lon", None, None), P(), P(), P(), P(), P(), P(), P(), P())
    out_specs = P("lat", "lon", None, None)
    return jax.shard_map(
        functools.partial(per_device, mesh.shape["lon"], mesh.shape["lat"]),
        mesh=mesh, in_specs=in_specs, out_specs=out_specs, check_vma=False,
    )
```
